32 devices in a mesh: col: 8 (over z, y), grp: 4 (over x, core).
Axes of the slice: x: 2, y: 2, z: 4, core: 2. Of those that a mesh axis runs over, the one named last changes fastest.
Arguments:
- density_now: float32 [2, 8192, 768], P(None, ('col', 'grp')), may hold values from -6 to 6
- density_before: float32 [2, 8192, 768], P(None, ('col', 'grp')), may hold values from -6 to 6
- source: float32 [2, 8192, 768], P(None, ('col', 'grp')), may hold values from -8 to 8
- response: float32 [8192, 768], P(('col', 'grp')), may hold values from 0.5 to 4
- history_density: bfloat16 [7, 2, 8192, 768], P(None, None, ('col', 'grp')), may hold values from -6 to 6
- history_residual: bfloat16 [7, 2, 8192, 768], P(None, None, ('col', 'grp')), may hold values from -6 to 6
- column_shell: int32 [8192], P(('col', 'grp')), may hold values from 1 to 139264, as said below
- screening: float32 [1], replicated, may hold values from 1466 to 36672
Outputs:
- slab_density: float32 [2, 2, 768, 8192], P(None, None, 'col', 'grp')
- mixed_density: float32 [2, 8192, 768], P(None, ('col', 'grp'))
- residual_norm: float32 [2], replicated
The draws below stay inside these ranges and needn't reach their ends.
Inputs may be any that keep to these rules, and one draw needn't show every extreme that they name: `column_shell`: column j's value lies between 1 + j * s and (j + 1) * s, where s = (383^2 - 1) // 8192.
All inputs are finite; a program needn't handle non-finite values.
Results may differ from the reference program's by a relative error of at most 0.0038.
Values sent between devices are 32-bit elements; how exact they have to be, the bound alone decides.
A program may use at most 192 MiB of HBM per device.

```python
import math
import jax
import jax.numpy as jnp
from jax import lax

NZ = 768
COL_DEV = 256
HIST = 8
ITERS = 2
COLS = 8192
CUT2 = 146689
N_COL = 8
N_GRP = 4


def normal_part(key, tag, shape):
    return jax.random.truncated_normal(jax.random.fold_in(key, tag), -4.0, 4.0, shape, jnp.float32)


def response_field(key):
    return jnp.exp(jax.random.uniform(jax.random.fold_in(key, 1), (COLS, NZ), jnp.float32, math.log(0.5), math.log(4.0)))


def history_coefficients(key):
    return jax.random.uniform(jax.random.fold_in(key, 2), (HIST - 1,), jnp.float32, -1.0, 1.0)


def step_entry(key, position):
    summed = 0.6 * normal_part(jax.random.fold_in(key, 3), position, (2, COLS, NZ))
    return summed


def fixed_point(key):
    return normal_part(key, 6, (2, COLS, NZ))


def current_density(key):
    coeffs = history_coefficients(key)
    summed = fixed_point(key) + 0.3 * normal_part(key, 7, (2, COLS, NZ))
    for position in range(HIST - 1):
        summed = summed + coeffs[position] * step_entry(key, position)
    return jnp.clip(summed, -6.0, 6.0)


def draw_density_now(key, part):
    return current_density(key)


def draw_density_before(key, part):
    summed = current_density(key) + 0.5 * normal_part(key, 8, (2, COLS, NZ))
    return jnp.clip(summed, -6.0, 6.0)


def draw_source(key, part):
    return jnp.clip(response_field(key)[None] * fixed_point(key), -8.0, 8.0)


def draw_response(key, part):
    return response_field(key)


def draw_history_density(key, part):
    entries = [step_entry(key, position) for position in range(HIST - 1)]
    return jnp.clip(jnp.stack(entries), -6.0, 6.0).astype(jnp.bfloat16)


def draw_history_residual(key, part):
    stiffness = response_field(key)
    entries = []
    for position in range(HIST - 1):
        noise = 0.3 * normal_part(jax.random.fold_in(key, 5), position, (2, COLS, NZ))
        entries.append(noise - stiffness[None] * step_entry(key, position))
    return jnp.clip(jnp.stack(entries), -6.0, 6.0).astype(jnp.bfloat16)


def draw_column_shell(key, part):
    radius_squared = (NZ // 2 - 1) ** 2
    spacing = (radius_squared - 1) // COLS
    lowest = 1 + jnp.arange(COLS, dtype=jnp.int32) * spacing
    return lowest + jax.random.randint(jax.random.fold_in(key, 9), (COLS,), 0, spacing, jnp.int32)


def setup_inputs(seed: int = 0) -> dict:
    keys = jax.random.split(jax.random.key(seed), 9)
    return {
        "density_now": draw_density_now(jax.random.fold_in(keys[8], 71), 0),
        "density_before": draw_density_before(jax.random.fold_in(keys[8], 71), 0),
        "source": draw_source(jax.random.fold_in(keys[8], 71), 0),
        "response": draw_response(jax.random.fold_in(keys[8], 71), 0),
        "history_density": draw_history_density(jax.random.fold_in(keys[8], 71), 0),
        "history_residual": draw_history_residual(jax.random.fold_in(keys[8], 71), 0),
        "column_shell": draw_column_shell(jax.random.fold_in(keys[8], 71), 0),
        "screening": jnp.clip(jnp.exp(jax.random.uniform(keys[7], (1,), jnp.float32, math.log(1466.0), math.log(36672.0))), 1466.0, 36672.0),
    }


MIXING = 0.7

def rounded(values):
    return lax.optimization_barrier(values.astype(jnp.bfloat16)).astype(jnp.float32)

def reference(density_now, density_before, source, response, history_density, history_residual, column_shell, screening):
    midpoint = NZ // 2
    slot_index = jnp.arange(NZ, dtype=jnp.int32)
    signed = jnp.where(slot_index < midpoint, slot_index, slot_index - NZ)
    squared = column_shell[:, None] + signed[None, :] * signed[None, :]
    inside = squared <= CUT2
    shells = squared.astype(jnp.float32)
    screen = screening[0]
    precond = MIXING * shells / (shells + screen)
    metric = jnp.where(inside, (shells + screen) / shells, jnp.float32(0.0))
    inside_mask = inside.astype(jnp.float32)
    weight_total = jnp.sum(metric)
    history_rho = [history_density[position] for position in range(HIST - 1)]
    history_res = [history_residual[position] for position in range(HIST - 1)]
    prev_residual = source - response[None] * density_before
    density = density_now
    previous = density_before
    slab_list = []
    norm_list = []
    for iteration in range(ITERS):
        residual = source - response[None] * density
        history_rho.append((density - previous).astype(jnp.bfloat16))
        history_res.append((residual - prev_residual).astype(jnp.bfloat16))
        if len(history_rho) > HIST:
            history_rho = history_rho[1:]
            history_res = history_res[1:]
        residual_half = rounded(residual)
        margin_rows = []
        projections = []
        for first_entry in history_res:
            weighted = rounded(metric[None] * first_entry.astype(jnp.float32))
            margin_rows.append(jnp.stack([jnp.sum(weighted * second_entry.astype(jnp.float32)) for second_entry in history_res]))
            projections.append(jnp.sum(weighted * residual_half))
        margin = jnp.stack(margin_rows)
        projection = jnp.stack(projections)
        square = jnp.sum(metric[None] * residual * residual)
        symmetric = 0.5 * (margin + margin.T)
        factor = jnp.linalg.cholesky(symmetric)
        coefficient = jax.scipy.linalg.cho_solve((factor, True), projection)
        norm_list.append(jnp.sqrt(square / weight_total))
        rho_mix = density
        res_mix = residual
        for position in range(HIST):
            rho_mix = rho_mix - coefficient[position] * history_rho[position].astype(jnp.float32)
            res_mix = res_mix - coefficient[position] * history_res[position].astype(jnp.float32)
        new_density = inside_mask[None] * (rho_mix + precond[None] * res_mix)
        spectrum = lax.complex(new_density[0], new_density[1])
        field = jnp.fft.ifft(spectrum, axis=-1) * math.sqrt(NZ)
        planes = jnp.stack([jnp.real(field).T, jnp.imag(field).T]).astype(jnp.float32)
        planes = planes.reshape(2, NZ, N_COL, N_GRP, COL_DEV).transpose(0, 1, 3, 2, 4).reshape(2, NZ, COLS)
        slab_list.append(planes)
        previous = density
        prev_residual = residual
        density = new_density
    return (jnp.stack(slab_list), density, jnp.stack(norm_list))
```

```python
import functools
import math

import jax
import jax.numpy as jnp
import numpy as np
from jax import lax
from jax.experimental import pallas as pl
from jax.experimental.pallas import tpu as pltpu
from jax.sharding import PartitionSpec as P

HIST = 8
ITERS = 2
MIXING = 0.7
ROWS = 16
CHUNK = 32
EARLY = 3
MESH = pl.DeviceIdType.MESH


def plane_table(plane_count, parts):
    slot = np.arange(plane_count)
    angle = (slot[:, None] * slot[None, :] % plane_count) * (2.0 * np.pi / plane_count)
    table = np.stack([np.cos(angle), np.sin(angle)])
    table = table.reshape(2, parts, plane_count // parts, plane_count).transpose(1, 0, 2, 3)
    table = table.reshape(parts, 2 * plane_count // parts, plane_count)
    return jnp.asarray(table.astype(np.float32)).astype(jnp.bfloat16)


def dot_rows(first, second):
    return lax.dot_general(
        first, second, (((1,), (1,)), ((), ())), preferred_element_type=jnp.float32
    )


def mix_kernel(
    n_col,
    n_grp,
    now_hbm,
    before_hbm,
    source_hbm,
    response_hbm,
    hist_rho_hbm,
    hist_res_hbm,
    shell_ref,
    screen_ref,
    table_hbm,
    slab_hbm,
    mixed_hbm,
    norm_ref,
    dens,
    source,
    response,
    rho,
    res,
    table,
    metric,
    precond,
    high,
    low,
    coef,
    gram,
    square,
    sums,
    outgoing,
    load_sem,
    late_sem,
    sums_send,
    sums_recv,
    slab_send,
    slab_recv,
    own_sem,
):
    columns, planes = response.shape
    slab = planes // n_col
    devices = n_col * n_grp
    col = lax.axis_index("col")
    grp = lax.axis_index("grp")
    me = col * n_grp + grp
    chunks = columns // CHUNK

    def peer_at(offset):
        peer = (me + offset) % devices
        return (peer // n_grp, peer % n_grp)

    barrier = pltpu.get_barrier_semaphore()

    def greet(offset, carry):
        pl.semaphore_signal(barrier, inc=1, device_id=peer_at(offset), device_id_type=MESH)
        return carry

    lax.fori_loop(1, devices, greet, 0)

    def load_copies(chunk):
        rows = pl.ds(pl.multiple_of(chunk * CHUNK, CHUNK), CHUNK)
        pairs = (
            (hist_res_hbm.at[:, :, rows, :], res.at[pl.ds(0, HIST - 1), :, rows, :]),
            (now_hbm.at[:, rows, :], dens.at[1, :, rows, :]),
            (before_hbm.at[:, rows, :], dens.at[0, :, rows, :]),
            (source_hbm.at[:, rows, :], source.at[:, rows, :]),
            (response_hbm.at[rows, :], response.at[rows, :]),
        )
        return [
            pltpu.make_async_copy(src, dst, load_sem.at[chunk, slot])
            for slot, (src, dst) in enumerate(pairs)
        ]

    def start_loads(chunk, carry):
        for copy in load_copies(chunk):
            copy.start()
        return carry

    lax.fori_loop(0, chunks, start_loads, 0)
    late_copies = (
        pltpu.make_async_copy(hist_rho_hbm, rho.at[pl.ds(0, HIST - 1)], late_sem.at[0]),
        pltpu.make_async_copy(table_hbm, table, late_sem.at[1]),
    )
    for copy in late_copies:
        copy.start()

    screen = screen_ref[0]

    def geometry(block, total):
        rows = pl.ds(pl.multiple_of(block * ROWS, ROWS), ROWS)
        slot = lax.broadcasted_iota(jnp.int32, (ROWS, planes), 1)
        signed = jnp.where(slot < planes // 2, slot, slot - planes)
        squared = shell_ref[rows, :] + signed * signed
        limit = (planes // 2 - 1) * (planes // 2 - 1)
        shells = squared.astype(jnp.float32)
        shifted = shells + screen
        value = jnp.where(squared <= limit, shifted / shells, jnp.float32(0.0))
        metric[rows, :] = value
        precond[rows, :] = MIXING * shells / shifted
        return total + value

    weights = lax.fori_loop(
        0, columns // ROWS, geometry, jnp.zeros((ROWS, planes), jnp.float32)
    )

    def whole_sum(values):
        return jnp.sum(jnp.sum(values, axis=0, keepdims=True), axis=1, keepdims=True)

    weight_local = whole_sum(weights)

    lane = lax.broadcasted_iota(jnp.int32, (HIST, 128), 1)
    row = lax.broadcasted_iota(jnp.int32, (HIST, 128), 0)

    def column_of(values, index):
        return jnp.sum(jnp.where(lane == index, values, 0.0), axis=1, keepdims=True)

    def statistics(t):
        gram[...] = jnp.zeros_like(gram)
        square[...] = jnp.zeros_like(square)

        def chunk_step(chunk, carry):
            if t == 0:
                for copy in load_copies(chunk):
                    copy.wait()
            for block in range(CHUNK // ROWS):
                rows = pl.ds(pl.multiple_of(chunk * CHUNK + block * ROWS, ROWS), ROWS)
                weight = metric[rows, :]
                gain = response[rows, :]
                for part in range(2):
                    current = dens[t + 1, part, rows, :]
                    previous = dens[t, part, rows, :]
                    constant = source[part, rows, :]
                    residual = constant - gain * current
                    earlier = constant - gain * previous
                    rho[t + HIST - 1, part, rows, :] = (current - previous).astype(jnp.bfloat16)
                    newest = (residual - earlier).astype(jnp.bfloat16)
                    res[t + HIST - 1, part, rows, :] = newest
                    stack = jnp.concatenate(
                        [res[pl.ds(t, HIST - 1), part, rows, :], newest[None]], axis=0
                    )
                    weighted = (weight[None] * stack.astype(jnp.float32)).astype(jnp.bfloat16)
                    right = jnp.concatenate(
                        [stack, residual.astype(jnp.bfloat16)[None]], axis=0
                    )
                    gram[...] += dot_rows(
                        weighted.reshape(HIST * ROWS, planes),
                        right.reshape((HIST + 1) * ROWS, planes),
                    )
                    square[...] += weight * residual * residual
            return carry

        lax.fori_loop(0, chunks, chunk_step, 0)
        shape = gram.shape
        same = (
            lax.broadcasted_iota(jnp.int32, shape, 0) % ROWS
            == lax.broadcasted_iota(jnp.int32, shape, 1) % ROWS
        )
        folded = jnp.where(same, gram[...], 0.0).reshape(HIST, ROWS, shape[1]).sum(axis=1)
        entry = lax.broadcasted_iota(jnp.int32, folded.shape, 1) // ROWS
        partial = jnp.zeros((HIST, 128), jnp.float32)
        for index in range(HIST + 1):
            total = jnp.sum(jnp.where(entry == index, folded, 0.0), axis=1, keepdims=True)
            partial = jnp.where(lane == index, total, partial)
        partial = jnp.where(lane == HIST + 1, whole_sum(square[...]), partial)
        partial = jnp.where(lane == HIST + 2, weight_local, partial)
        sums[t, me] = partial

    def sum_copy(t, offset, slot):
        return pltpu.make_async_remote_copy(
            src_ref=sums.at[t, me],
            dst_ref=sums.at[t, slot],
            send_sem=sums_send.at[t, offset],
            recv_sem=sums_recv.at[t, offset],
            device_id=peer_at(offset),
            device_id_type=MESH,
        )

    def send_sums(t):
        def step(offset, carry):
            sum_copy(t, offset, me).start()
            return carry

        lax.fori_loop(1, devices, step, 0)

    def take_sums(t):
        def step(offset, carry):
            sum_copy(t, offset, (me - offset + devices) % devices).wait()
            return carry

        lax.fori_loop(1, devices, step, 0)

    def solve(t):
        total = jnp.sum(sums[t], axis=0)
        norm_ref[pl.ds(t, 1), :] = jnp.broadcast_to(
            jnp.sqrt(column_of(total, HIST + 1) / column_of(total, HIST + 2))[:1], (1, 128)
        )
        flipped = jnp.concatenate([total] * (128 // HIST), axis=0).T[:HIST]
        system = jnp.where(lane < HIST, 0.5 * (total + flipped), total)
        for pivot in range(HIST):
            pivot_row = jnp.sum(jnp.where(row == pivot, system, 0.0), axis=0, keepdims=True)
            root = jnp.sqrt(
                jnp.sum(jnp.where(lane[:1] == pivot, pivot_row, 0.0), axis=1, keepdims=True)
            )
            factor = column_of(system, pivot) / root
            system = jnp.where(row == pivot, system, system - factor * (pivot_row / root))
        diagonal = jnp.sum(jnp.where(lane == row, system, 0.0), axis=1, keepdims=True)
        coef[...] = jnp.broadcast_to(column_of(system, HIST) / diagonal, coef.shape)

    def update(t):
        def block_step(block, carry):
            rows = pl.ds(pl.multiple_of(block * ROWS, ROWS), ROWS)
            inside = metric[rows, :] > 0.0
            gain = response[rows, :]
            scale = precond[rows, :]
            for part in range(2):
                current = dens[t + 1, part, rows, :]
                rho_mix = current
                res_mix = source[part, rows, :] - gain * current
                for entry in range(HIST):
                    weight = coef[pl.ds(entry, 1), :]
                    rho_mix = rho_mix - weight * rho[t + entry, part, rows, :].astype(jnp.float32)
                    res_mix = res_mix - weight * res[t + entry, part, rows, :].astype(jnp.float32)
                fresh = jnp.where(inside, rho_mix + scale * res_mix, 0.0)
                dens[t + 2, part, rows, :] = fresh
                top = fresh.astype(jnp.bfloat16)
                spot = pl.ds(pl.multiple_of(part * columns + block * ROWS, ROWS), ROWS)
                high[spot, :] = top
                low[spot, :] = (fresh - top.astype(jnp.float32)).astype(jnp.bfloat16)
            return carry

        lax.fori_loop(0, columns // ROWS, block_step, 0)

    def slab_copy(t, offset, origin):
        target = (col + offset) % n_col
        return pltpu.make_async_remote_copy(
            src_ref=outgoing.at[t, offset],
            dst_ref=slab_hbm.at[t, :, :, pl.ds(pl.multiple_of(origin * columns, 128), columns)],
            send_sem=slab_send.at[t, offset],
            recv_sem=slab_recv.at[t, offset],
            device_id=(target, grp),
            device_id_type=MESH,
        )

    def own_copy(t):
        return pltpu.make_async_copy(
            outgoing.at[t, 0],
            slab_hbm.at[t, :, :, pl.ds(pl.multiple_of(col * columns, 128), columns)],
            own_sem.at[t],
        )

    def transform(t, offset):
        lines = table[(col + offset) % n_col]
        products = dot_rows(lines, high[...]) + dot_rows(lines, low[...])
        products = products * jnp.float32(1.0 / math.sqrt(planes))
        cosine = products[:slab]
        sine = products[slab:]
        outgoing[t, offset, 0] = cosine[:, :columns] - sine[:, columns:]
        outgoing[t, offset, 1] = sine[:, :columns] + cosine[:, columns:]

    def send_slabs(t, first, last):
        def step(index, carry):
            offset = n_col // 2 + (1 - 2 * (index % 2)) * ((index + 1) // 2)
            transform(t, offset)
            slab_copy(t, offset, col).start()
            return carry

        lax.fori_loop(first, last, step, 0)

    statistics(0)
    pl.semaphore_wait(barrier, devices - 1)
    send_sums(0)
    for copy in late_copies:
        copy.wait()
    take_sums(0)
    solve(0)
    update(0)
    send_slabs(0, 0, EARLY)
    statistics(1)
    send_sums(1)
    send_slabs(0, EARLY, n_col - 1)
    transform(0, 0)
    own_copy(0).start()
    take_sums(1)
    solve(1)
    update(1)
    mixed_copy = pltpu.make_async_copy(dens.at[ITERS + 1], mixed_hbm, own_sem.at[ITERS])
    mixed_copy.start()
    send_slabs(1, 0, n_col - 1)
    transform(1, 0)
    own_copy(1).start()

    for t in range(ITERS):

        def finish(offset, carry):
            slab_copy(t, offset, (col - offset + n_col) % n_col).wait()
            return carry

        lax.fori_loop(1, n_col, finish, 0)
        own_copy(t).wait()
    mixed_copy.wait()


def body(
    n_col,
    n_grp,
    density_now,
    density_before,
    source,
    response,
    history_density,
    history_residual,
    column_shell,
    screening,
):
    _, columns, planes = density_now.shape
    slab = planes // n_col
    devices = n_col * n_grp
    table = plane_table(planes, n_col)
    f32, bf16 = jnp.float32, jnp.bfloat16
    any_space = pl.BlockSpec(memory_space=pl.ANY)
    vmem_space = pl.BlockSpec(memory_space=pltpu.VMEM)
    slab_out, mixed, norms = pl.pallas_call(
        functools.partial(mix_kernel, n_col, n_grp),
        out_shape=(
            jax.ShapeDtypeStruct((ITERS, 2, slab, n_col * columns), f32),
            jax.ShapeDtypeStruct((2, columns, planes), f32),
            jax.ShapeDtypeStruct((8, 128), f32),
        ),
        in_specs=[any_space] * 6
        + [vmem_space, pl.BlockSpec(memory_space=pltpu.SMEM), any_space],
        out_specs=(any_space, any_space, vmem_space),
        scratch_shapes=[
            pltpu.VMEM((ITERS + 2, 2, columns, planes), f32),
            pltpu.VMEM((2, columns, planes), f32),
            pltpu.VMEM((columns, planes), f32),
            pltpu.VMEM((HIST + ITERS - 1, 2, columns, planes), bf16),
            pltpu.VMEM((HIST + ITERS - 1, 2, columns, planes), bf16),
            pltpu.VMEM(table.shape, bf16),
            pltpu.VMEM((columns, planes), f32),
            pltpu.VMEM((columns, planes), f32),
            pltpu.VMEM((2 * columns, planes), bf16),
            pltpu.VMEM((2 * columns, planes), bf16),
            pltpu.VMEM((HIST, planes), f32),
            pltpu.VMEM((HIST * ROWS, (HIST + 1) * ROWS), f32),
            pltpu.VMEM((ROWS, planes), f32),
            pltpu.VMEM((ITERS, devices, HIST, 128), f32),
            pltpu.VMEM((ITERS, n_col, 2, slab, columns), f32),
            pltpu.SemaphoreType.DMA((columns // CHUNK, 5)),
            pltpu.SemaphoreType.DMA((2,)),
            pltpu.SemaphoreType.DMA((ITERS, devices)),
            pltpu.SemaphoreType.DMA((ITERS, devices)),
            pltpu.SemaphoreType.DMA((ITERS, n_col)),
            pltpu.SemaphoreType.DMA((ITERS, n_col)),
            pltpu.SemaphoreType.DMA((ITERS + 1,)),
        ],
        compiler_params=pltpu.CompilerParams(
            collective_id=0, has_side_effects=True, vmem_limit_bytes=60 * 1024 * 1024
        ),
    )(
        density_now,
        density_before,
        source,
        response,
        history_density,
        history_residual,
        column_shell[:, None],
        screening,
        table,
    )
    return (slab_out, mixed, norms[:ITERS, 0])


def solution(mesh):
    return jax.shard_map(
        functools.partial(body, mesh.shape["col"], mesh.shape["grp"]),
        mesh=mesh,
        in_specs=(
            P(None, ("col", "grp"), None),
            P(None, ("col", "grp"), None),
            P(None, ("col", "grp"), None),
            P(("col", "grp"), None),
            P(None, None, ("col", "grp"), None),
            P(None, None, ("col", "grp"), None),
            P(("col", "grp")),
            P(),
        ),
        out_specs=(P(None, None, "col", "grp"), P(None, ("col", "grp"), None), P()),
        check_vma=False,
    )
```

```python
import functools
import math

import jax
import jax.numpy as jnp
import numpy as np
from jax import lax
from jax.experimental import pallas as pl
from jax.experimental.pallas import tpu as pltpu
from jax.sharding import PartitionSpec as P

HIST = 8
ITERS = 2
MIXING = 0.7
ROWS = 16
CHUNK = 32
EARLY = 3
MESH = pl.DeviceIdType.MESH


def plane_table(plane_count, parts):
    slot = np.arange(plane_count)
    angle = (slot[:, None] * slot[None, :] % plane_count) * (2.0 * np.pi / plane_count)
    table = np.stack([np.cos(angle), np.sin(angle)])
    table = table.reshape(2, parts, plane_count // parts, plane_count).transpose(1, 0, 2, 3)
    table = table.reshape(parts, 2 * plane_count // parts, plane_count)
    return jnp.asarray(table.astype(np.float32)).astype(jnp.bfloat16)


def dot_rows(first, second):
    return lax.dot_general(
        first, second, (((1,), (1,)), ((), ())), preferred_element_type=jnp.float32
    )


def mix_kernel(
    n_col,
    n_grp,
    now_hbm,
    before_hbm,
    source_hbm,
    response_hbm,
    hist_rho_hbm,
    hist_res_hbm,
    shell_ref,
    screen_ref,
    table_hbm,
    slab_hbm,
    mixed_hbm,
    norm_ref,
    dens,
    source,
    response,
    rho,
    res,
    table,
    metric,
    precond,
    high,
    low,
    coef,
    gram,
    square,
    shells_down,
    sums,
    outgoing,
    load_sem,
    late_sem,
    sums_send,
    sums_recv,
    slab_send,
    slab_recv,
    own_sem,
):
    columns, planes = response.shape
    slab = planes // n_col
    devices = n_col * n_grp
    col = lax.axis_index("col")
    grp = lax.axis_index("grp")
    me = col * n_grp + grp
    chunks = columns // CHUNK

    def peer_at(offset):
        peer = (me + offset) % devices
        return (peer // n_grp, peer % n_grp)

    barrier = pltpu.get_barrier_semaphore()

    def greet(offset, carry):
        pl.semaphore_signal(barrier, inc=1, device_id=peer_at(offset), device_id_type=MESH)
        return carry

    lax.fori_loop(1, devices, greet, 0)

    def load_copies(chunk):
        rows = pl.ds(pl.multiple_of(chunk * CHUNK, CHUNK), CHUNK)
        pairs = (
            (hist_res_hbm.at[:, :, rows, :], res.at[pl.ds(0, HIST - 1), :, rows, :]),
            (now_hbm.at[:, rows, :], dens.at[1, :, rows, :]),
            (before_hbm.at[:, rows, :], dens.at[0, :, rows, :]),
            (source_hbm.at[:, rows, :], source.at[:, rows, :]),
            (response_hbm.at[rows, :], response.at[rows, :]),
        )
        return [
            pltpu.make_async_copy(src, dst, load_sem.at[chunk, slot])
            for slot, (src, dst) in enumerate(pairs)
        ]

    def start_loads(chunk, carry):
        for copy in load_copies(chunk):
            copy.start()
        return carry

    lax.fori_loop(0, chunks, start_loads, 0)
    late_copies = (
        pltpu.make_async_copy(hist_rho_hbm, rho.at[pl.ds(0, HIST - 1)], late_sem.at[0]),
        pltpu.make_async_copy(table_hbm, table, late_sem.at[1]),
    )
    for copy in late_copies:
        copy.start()

    screen = screen_ref[0]
    shell_row = shell_ref[...].astype(jnp.float32)
    shells_down[...] = jnp.broadcast_to(shell_row, (128, columns)).T

    def geometry(block, total):
        rows = pl.ds(pl.multiple_of(block * ROWS, ROWS), ROWS)
        slot = lax.broadcasted_iota(jnp.int32, (ROWS, planes), 1)
        signed = jnp.where(slot < planes // 2, slot, slot - planes)
        squared = shells_down[rows, :1].astype(jnp.int32) + signed * signed
        limit = (planes // 2 - 1) * (planes // 2 - 1)
        shells = squared.astype(jnp.float32)
        shifted = shells + screen
        value = jnp.where(squared <= limit, shifted / shells, jnp.float32(0.0))
        metric[rows, :] = value
        precond[rows, :] = MIXING * shells / shifted
        return total + value

    weights = lax.fori_loop(
        0, columns // ROWS, geometry, jnp.zeros((ROWS, planes), jnp.float32)
    )

    def whole_sum(values):
        return jnp.sum(jnp.sum(values, axis=0, keepdims=True), axis=1, keepdims=True)

    weight_local = whole_sum(weights)

    lane = lax.broadcasted_iota(jnp.int32, (HIST, 128), 1)
    row = lax.broadcasted_iota(jnp.int32, (HIST, 128), 0)

    def column_of(values, index):
        return jnp.sum(jnp.where(lane == index, values, 0.0), axis=1, keepdims=True)

    def statistics(t):
        gram[...] = jnp.zeros_like(gram)
        square[...] = jnp.zeros_like(square)

        def chunk_step(chunk, carry):
            if t == 0:
                for copy in load_copies(chunk):
                    copy.wait()
            for block in range(CHUNK // ROWS):
                rows = pl.ds(pl.multiple_of(chunk * CHUNK + block * ROWS, ROWS), ROWS)
                weight = metric[rows, :]
                gain = response[rows, :]
                for part in range(2):
                    current = dens[t + 1, part, rows, :]
                    previous = dens[t, part, rows, :]
                    constant = source[part, rows, :]
                    residual = constant - gain * current
                    earlier = constant - gain * previous
                    rho[t + HIST - 1, part, rows, :] = (current - previous).astype(jnp.bfloat16)
                    newest = (residual - earlier).astype(jnp.bfloat16)
                    res[t + HIST - 1, part, rows, :] = newest
                    stack = jnp.concatenate(
                        [res[pl.ds(t, HIST - 1), part, rows, :], newest[None]], axis=0
                    )
                    weighted = (weight[None] * stack.astype(jnp.float32)).astype(jnp.bfloat16)
                    right = jnp.concatenate(
                        [stack, residual.astype(jnp.bfloat16)[None]], axis=0
                    )
                    gram[...] += dot_rows(
                        weighted.reshape(HIST * ROWS, planes),
                        right.reshape((HIST + 1) * ROWS, planes),
                    )
                    square[...] += weight * residual * residual
            return carry

        lax.fori_loop(0, chunks, chunk_step, 0)
        shape = gram.shape
        same = (
            lax.broadcasted_iota(jnp.int32, shape, 0) % ROWS
            == lax.broadcasted_iota(jnp.int32, shape, 1) % ROWS
        )
        folded = jnp.where(same, gram[...], 0.0).reshape(HIST, ROWS, shape[1]).sum(axis=1)
        entry = lax.broadcasted_iota(jnp.int32, folded.shape, 1) // ROWS
        partial = jnp.zeros((HIST, 128), jnp.float32)
        for index in range(HIST + 1):
            total = jnp.sum(jnp.where(entry == index, folded, 0.0), axis=1, keepdims=True)
            partial = jnp.where(lane == index, total, partial)
        partial = jnp.where(lane == HIST + 1, whole_sum(square[...]), partial)
        partial = jnp.where(lane == HIST + 2, weight_local, partial)
        sums[t, me] = partial

    def sum_copy(t, offset, slot):
        return pltpu.make_async_remote_copy(
            src_ref=sums.at[t, me],
            dst_ref=sums.at[t, slot],
            send_sem=sums_send.at[t, offset],
            recv_sem=sums_recv.at[t, offset],
            device_id=peer_at(offset),
            device_id_type=MESH,
        )

    def send_sums(t):
        def step(offset, carry):
            sum_copy(t, offset, me).start()
            return carry

        lax.fori_loop(1, devices, step, 0)

    def take_sums(t):
        def step(offset, carry):
            sum_copy(t, offset, (me - offset + devices) % devices).wait()
            return carry

        lax.fori_loop(1, devices, step, 0)

    def solve(t):
        total = jnp.sum(sums[t], axis=0)
        norm = jnp.sqrt(column_of(total, HIST + 1) / column_of(total, HIST + 2))
        norm_ref[t] = norm[0, 0]
        flipped = jnp.concatenate([total] * (128 // HIST), axis=0).T[:HIST]
        system = jnp.where(lane < HIST, 0.5 * (total + flipped), total)
        for pivot in range(HIST):
            pivot_row = jnp.sum(jnp.where(row == pivot, system, 0.0), axis=0, keepdims=True)
            root = jnp.sqrt(
                jnp.sum(jnp.where(lane[:1] == pivot, pivot_row, 0.0), axis=1, keepdims=True)
            )
            factor = column_of(system, pivot) / root
            system = jnp.where(row == pivot, system, system - factor * (pivot_row / root))
        diagonal = jnp.sum(jnp.where(lane == row, system, 0.0), axis=1, keepdims=True)
        coef[...] = jnp.broadcast_to(column_of(system, HIST) / diagonal, coef.shape)

    def update(t):
        def block_step(block, carry):
            rows = pl.ds(pl.multiple_of(block * ROWS, ROWS), ROWS)
            inside = metric[rows, :] > 0.0
            gain = response[rows, :]
            scale = precond[rows, :]
            for part in range(2):
                current = dens[t + 1, part, rows, :]
                rho_mix = current
                res_mix = source[part, rows, :] - gain * current
                for entry in range(HIST):
                    weight = coef[pl.ds(entry, 1), :]
                    rho_mix = rho_mix - weight * rho[t + entry, part, rows, :].astype(jnp.float32)
                    res_mix = res_mix - weight * res[t + entry, part, rows, :].astype(jnp.float32)
                fresh = jnp.where(inside, rho_mix + scale * res_mix, 0.0)
                dens[t + 2, part, rows, :] = fresh
                top = fresh.astype(jnp.bfloat16)
                spot = pl.ds(pl.multiple_of(part * columns + block * ROWS, ROWS), ROWS)
                high[spot, :] = top
                low[spot, :] = (fresh - top.astype(jnp.float32)).astype(jnp.bfloat16)
            return carry

        lax.fori_loop(0, columns // ROWS, block_step, 0)

    def slab_copy(t, offset, origin):
        target = (col + offset) % n_col
        return pltpu.make_async_remote_copy(
            src_ref=outgoing.at[t, offset],
            dst_ref=slab_hbm.at[t, :, :, pl.ds(pl.multiple_of(origin * columns, 128), columns)],
            send_sem=slab_send.at[t, offset],
            recv_sem=slab_recv.at[t, offset],
            device_id=(target, grp),
            device_id_type=MESH,
        )

    def own_copy(t):
        return pltpu.make_async_copy(
            outgoing.at[t, 0],
            slab_hbm.at[t, :, :, pl.ds(pl.multiple_of(col * columns, 128), columns)],
            own_sem.at[t],
        )

    def transform(t, offset):
        lines = table[(col + offset) % n_col]
        products = dot_rows(lines, high[...]) + dot_rows(lines, low[...])
        products = products * jnp.float32(1.0 / math.sqrt(planes))
        cosine = products[:slab]
        sine = products[slab:]
        outgoing[t, offset, 0] = cosine[:, :columns] - sine[:, columns:]
        outgoing[t, offset, 1] = sine[:, :columns] + cosine[:, columns:]

    def send_slabs(t, first, last):
        def step(index, carry):
            offset = n_col // 2 + (1 - 2 * (index % 2)) * ((index + 1) // 2)
            transform(t, offset)
            slab_copy(t, offset, col).start()
            return carry

        lax.fori_loop(first, last, step, 0)

    statistics(0)
    pl.semaphore_wait(barrier, devices - 1)
    send_sums(0)
    for copy in late_copies:
        copy.wait()
    take_sums(0)
    solve(0)
    update(0)
    send_slabs(0, 0, EARLY)
    statistics(1)
    send_sums(1)
    send_slabs(0, EARLY, n_col - 1)
    transform(0, 0)
    own_copy(0).start()
    take_sums(1)
    solve(1)
    update(1)
    mixed_copy = pltpu.make_async_copy(dens.at[ITERS + 1], mixed_hbm, own_sem.at[ITERS])
    mixed_copy.start()
    send_slabs(1, 0, n_col - 1)
    transform(1, 0)
    own_copy(1).start()

    for t in range(ITERS):

        def finish(offset, carry):
            slab_copy(t, offset, (col - offset + n_col) % n_col).wait()
            return carry

        lax.fori_loop(1, n_col, finish, 0)
        own_copy(t).wait()
    mixed_copy.wait()


def body(
    n_col,
    n_grp,
    density_now,
    density_before,
    source,
    response,
    history_density,
    history_residual,
    column_shell,
    screening,
):
    _, columns, planes = density_now.shape
    slab = planes // n_col
    devices = n_col * n_grp
    table = plane_table(planes, n_col)
    f32, bf16 = jnp.float32, jnp.bfloat16
    any_space = pl.BlockSpec(memory_space=pl.ANY)
    vmem_space = pl.BlockSpec(memory_space=pltpu.VMEM)
    slab_out, mixed, norms = pl.pallas_call(
        functools.partial(mix_kernel, n_col, n_grp),
        out_shape=(
            jax.ShapeDtypeStruct((ITERS, 2, slab, n_col * columns), f32),
            jax.ShapeDtypeStruct((2, columns, planes), f32),
            jax.ShapeDtypeStruct((ITERS,), f32),
        ),
        in_specs=[any_space] * 6
        + [vmem_space, pl.BlockSpec(memory_space=pltpu.SMEM), any_space],
        out_specs=(any_space, any_space, pl.BlockSpec(memory_space=pltpu.SMEM)),
        scratch_shapes=[
            pltpu.VMEM((ITERS + 2, 2, columns, planes), f32),
            pltpu.VMEM((2, columns, planes), f32),
            pltpu.VMEM((columns, planes), f32),
            pltpu.VMEM((HIST + ITERS - 1, 2, columns, planes), bf16),
            pltpu.VMEM((HIST + ITERS - 1, 2, columns, planes), bf16),
            pltpu.VMEM(table.shape, bf16),
            pltpu.VMEM((columns, planes), f32),
            pltpu.VMEM((columns, planes), f32),
            pltpu.VMEM((2 * columns, planes), bf16),
            pltpu.VMEM((2 * columns, planes), bf16),
            pltpu.VMEM((HIST, planes), f32),
            pltpu.VMEM((HIST * ROWS, (HIST + 1) * ROWS), f32),
            pltpu.VMEM((ROWS, planes), f32),
            pltpu.VMEM((columns, 128), f32),
            pltpu.VMEM((ITERS, devices, HIST, 128), f32),
            pltpu.VMEM((ITERS, n_col, 2, slab, columns), f32),
            pltpu.SemaphoreType.DMA((columns // CHUNK, 5)),
            pltpu.SemaphoreType.DMA((2,)),
            pltpu.SemaphoreType.DMA((ITERS, devices)),
            pltpu.SemaphoreType.DMA((ITERS, devices)),
            pltpu.SemaphoreType.DMA((ITERS, n_col)),
            pltpu.SemaphoreType.DMA((ITERS, n_col)),
            pltpu.SemaphoreType.DMA((ITERS + 1,)),
        ],
        compiler_params=pltpu.CompilerParams(
            collective_id=0, has_side_effects=True, vmem_limit_bytes=60 * 1024 * 1024
        ),
    )(
        density_now,
        density_before,
        source,
        response,
        history_density,
        history_residual,
        column_shell[None, :],
        screening,
        table,
    )
    return (slab_out, mixed, norms)


def solution(mesh):
    return jax.shard_map(
        functools.partial(body, mesh.shape["col"], mesh.shape["grp"]),
        mesh=mesh,
        in_specs=(
            P(None, ("col", "grp"), None),
            P(None, ("col", "grp"), None),
            P(None, ("col", "grp"), None),
            P(("col", "grp"), None),
            P(None, None, ("col", "grp"), None),
            P(None, None, ("col", "grp"), None),
            P(("col", "grp")),
            P(),
        ),
        out_specs=(P(None, None, "col", "grp"), P(None, ("col", "grp"), None), P()),
        check_vma=False,
    )
```
